256 devices in a mesh: replica: 16 (over z, core), model: 4 (over x), shift: 4 (over y).
Axes of the slice: x: 4, y: 4, z: 8, core: 2. Of those that a mesh axis runs over, the one named last changes fastest.
Arguments:
- partial_gate: float32 [64, 1024, 3072], P(('shift', 'replica'), None, 'model'), parts along dimension 0, may hold values from -0.875 to 0.875
- partial_up: float32 [64, 1024, 3072], P(('shift', 'replica'), None, 'model'), parts along dimension 0, may hold values from -0.875 to 0.875
- partial_down: float32 [64, 3072, 1024], P(('shift', 'replica'), 'model'), parts along dimension 0, may hold values from -0.875 to 0.875
- partial_norm: float32 [64, 1024], P(('shift', 'replica')), parts along dimension 0, may hold values from -8 to 8
- master_gate: float32 [4096, 3072], P(('shift', 'replica'), 'model'), parts along dimension 0, may hold values from -0.25 to 0.25
- master_up: float32 [4096, 3072], P(('shift', 'replica'), 'model'), parts along dimension 0, may hold values from -0.25 to 0.25
- master_down: float32 [12288, 1024], P(('shift', 'model'), 'replica'), parts along dimension 0, may hold values from -0.15625 to 0.15625
- master_norm: float32 [4096], P(('shift', 'replica')), parts along dimension 0, may hold values from 0.25 to 1.75
- memory_gate: float32 [4096, 3072], P(('shift', 'replica'), 'model'), parts along dimension 0, may hold values from -0.1875 to 0.1875
- memory_up: float32 [4096, 3072], P(('shift', 'replica'), 'model'), parts along dimension 0, may hold values from -0.1875 to 0.1875
- memory_down: float32 [12288, 1024], P(('shift', 'model'), 'replica'), parts along dimension 0, may hold values from -0.109375 to 0.109375
- memory_norm: float32 [4096], P(('shift', 'replica')), parts along dimension 0, may hold values from -1.75 to 1.75
Outputs:
- compute_gate: bfloat16 [4096, 3072], P('shift', 'model'), parts along dimension 0
- compute_up: bfloat16 [4096, 3072], P('shift', 'model'), parts along dimension 0
- compute_down: bfloat16 [12288, 1024], P(('shift', 'model')), parts along dimension 0
- compute_norm: bfloat16 [4096], P('shift'), parts along dimension 0
- stepped_gate: float32 [4096, 3072], P(('shift', 'replica'), 'model'), parts along dimension 0
- stepped_up: float32 [4096, 3072], P(('shift', 'replica'), 'model'), parts along dimension 0
- stepped_down: float32 [12288, 1024], P(('shift', 'model'), 'replica'), parts along dimension 0
- stepped_norm: float32 [4096], P(('shift', 'replica')), parts along dimension 0
- state_new_gate: float32 [4096, 3072], P(('shift', 'replica'), 'model'), parts along dimension 0
- state_new_up: float32 [4096, 3072], P(('shift', 'replica'), 'model'), parts along dimension 0
- state_new_down: float32 [12288, 1024], P(('shift', 'model'), 'replica'), parts along dimension 0
- state_new_norm: float32 [4096], P(('shift', 'replica')), parts along dimension 0
The draws below stay inside these ranges and needn't reach their ends.
There are 4 independent parts, one for each index of `shift`. The reference program is written for one: setup_inputs(seed, part) draws one part's arguments, and reference() takes and returns one part's arrays. A program takes and returns all parts, laid end to end along the dimension named above; each array names one. Nothing has to cross between parts.
All inputs are finite; a program needn't handle non-finite values.
Results may differ from the reference program's by a relative error of at most 0.001.
Values may be sent and summed in bfloat16 or wider, within the bound.
A program may use at most 128 MiB of HBM per device.

```python
import jax
import jax.numpy as jnp
from jax import lax

WIDTH = 1024
INNER = 3072
REPLICAS = 16


def spiked(drawn, own_key, source, target, parts, factor):
    owner, partner = [(jnp.arange(drawn.shape[axis_at]) // (drawn.shape[axis_at] // parts)).reshape([-1 if axis == axis_at else 1 for axis in range(drawn.ndim)]) for axis_at in (source, target)]
    chosen = jax.random.permutation(own_key, parts)[partner]
    strong = (owner == chosen) | (owner == (partner + parts // 2) % parts)
    return jnp.where(strong, factor * drawn, drawn)


def steps_of(stream_key, dims, cuts, smallest, high):
    def one(position, blocks):
        steps = jax.random.uniform(jax.random.fold_in(jax.random.fold_in(stream_key, 6), position), (blocks,), jnp.float32, smallest / len(cuts), high / len(cuts))
        return jnp.repeat(jnp.exp(steps), dims[position] // blocks).reshape((-1,) + (1,) * (len(dims) - position - 1))

    loudness = one(*cuts[0])
    for cut in cuts[1:]:
        loudness = loudness * one(*cut)
    return loudness


def scatter_about(key, dims, deviation, most, pieces=(), dtype=jnp.bfloat16):
    factor_of = steps_of(key, dims, pieces, -0.22, 0.18) if pieces else 1.0
    values = jax.random.normal(key, dims, jnp.float32) * deviation * factor_of
    return jnp.minimum(jnp.maximum(values, -most), most).astype(dtype)


def noise_with(key, dims, scale, limit, split, heavy, kind=jnp.bfloat16):
    entries = scale * jax.random.normal(key, dims, jnp.float32)
    if split:
        entries = entries * steps_of(key, dims, split, -0.22, 0.18)
    return jnp.clip(spiked(entries, jax.random.fold_in(key, 3), *heavy), -limit, limit).astype(kind)


def setup_inputs(seed: int = 0, part: int = 0) -> dict:
    keys = jax.random.split(jax.random.key(seed), 13)
    part_splits = jax.random.split(jax.random.fold_in(keys[12], part), 13)
    partial_gate = noise_with(part_splits[0], (REPLICAS, WIDTH, INNER), 0.1, 0.875, ((0, 16), (2, 4)), (0, 1, 16, 2.0), jnp.float32)
    partial_up = noise_with(part_splits[1], (REPLICAS, WIDTH, INNER), 0.1, 0.875, ((0, 16), (2, 4)), (0, 1, 16, 2.0), jnp.float32)
    partial_down = noise_with(part_splits[2], (REPLICAS, INNER, WIDTH), 0.1, 0.875, ((0, 16), (1, 4)), (0, 2, 16, 2.0), jnp.float32)
    partial_norm = noise_with(part_splits[3], (REPLICAS, WIDTH), 1.0, 8.0, ((0, 16),), (0, 1, 16, 2.0), jnp.float32)
    master_gate = noise_with(part_splits[4], (WIDTH, INNER), WIDTH ** -0.5, 0.25, ((0, 16), (1, 4)), (1, 0, 16, 2.0), jnp.float32)
    master_up = noise_with(part_splits[5], (WIDTH, INNER), WIDTH ** -0.5, 0.25, ((0, 16), (1, 4)), (1, 0, 16, 2.0), jnp.float32)
    master_down = noise_with(part_splits[6], (INNER, WIDTH), INNER ** -0.5, 0.15625, ((0, 4), (1, 16)), (0, 1, 16, 2.0), jnp.float32)
    master_norm = jnp.clip(1.0 + 0.15 * jax.random.normal(part_splits[7], (WIDTH,), jnp.float32), 0.25, 1.75)
    memory_gate = scatter_about(part_splits[8], (WIDTH, INNER), WIDTH ** -0.5, 0.1875, ((0, 16), (1, 4)), jnp.float32)
    memory_up = scatter_about(part_splits[9], (WIDTH, INNER), WIDTH ** -0.5, 0.1875, ((0, 16), (1, 4)), jnp.float32)
    memory_down = scatter_about(part_splits[10], (INNER, WIDTH), INNER ** -0.5, 0.109375, ((0, 4), (1, 16)), jnp.float32)
    memory_norm = scatter_about(part_splits[11], (WIDTH,), 0.3, 1.75, ((0, 16),), jnp.float32)
    return {"partial_gate": partial_gate, "partial_up": partial_up, "partial_down": partial_down, "partial_norm": partial_norm, "master_gate": master_gate, "master_up": master_up, "master_down": master_down, "master_norm": master_norm, "memory_gate": memory_gate, "memory_up": memory_up, "memory_down": memory_down, "memory_norm": memory_norm}


learn_rate = 0.5
hold_rate = 0.9

def reference(partial_gate, partial_up, partial_down, partial_norm, master_gate, master_up, master_down, master_norm, memory_gate, memory_up, memory_down, memory_norm):
    mean_gate = lax.optimization_barrier(jnp.sum(partial_gate.astype(jnp.float32), axis=0)) * REPLICAS ** (-0.5)
    mean_up = lax.optimization_barrier(jnp.sum(partial_up.astype(jnp.float32), axis=0)) * REPLICAS ** (-0.5)
    mean_down = lax.optimization_barrier(jnp.sum(partial_down.astype(jnp.float32), axis=0)) * REPLICAS ** (-0.5)
    mean_norm = lax.optimization_barrier(jnp.sum(partial_norm.astype(jnp.float32), axis=0)) * REPLICAS ** (-0.5)
    ratio_gate = jnp.sqrt(lax.optimization_barrier(jnp.sum(master_gate * master_gate, axis=1, keepdims=True))) * lax.rsqrt(lax.optimization_barrier(jnp.sum(mean_gate * mean_gate, axis=1, keepdims=True)) + 1e-06)
    mean_gate = mean_gate * ratio_gate
    ratio_up = jnp.sqrt(lax.optimization_barrier(jnp.sum(master_up * master_up, axis=1, keepdims=True))) * lax.rsqrt(lax.optimization_barrier(jnp.sum(mean_up * mean_up, axis=1, keepdims=True)) + 1e-06)
    mean_up = mean_up * ratio_up
    ratio_down = jnp.sqrt(lax.optimization_barrier(jnp.sum(master_down * master_down, axis=0, keepdims=True))) * lax.rsqrt(lax.optimization_barrier(jnp.sum(mean_down * mean_down, axis=0, keepdims=True)) + 1e-06)
    mean_down = mean_down * ratio_down
    state_new_gate = hold_rate * memory_gate + mean_gate
    stepped_gate = master_gate - learn_rate * state_new_gate
    state_new_up = hold_rate * memory_up + mean_up
    stepped_up = master_up - learn_rate * state_new_up
    state_new_down = hold_rate * memory_down + mean_down
    stepped_down = master_down - learn_rate * state_new_down
    state_new_norm = hold_rate * memory_norm + mean_norm
    stepped_norm = master_norm - learn_rate * state_new_norm
    compute_gate = stepped_gate.astype(jnp.bfloat16)
    compute_up = stepped_up.astype(jnp.bfloat16)
    compute_down = stepped_down.astype(jnp.bfloat16)
    compute_norm = stepped_norm.astype(jnp.bfloat16)
    return (compute_gate, compute_up, compute_down, compute_norm, stepped_gate, stepped_up, stepped_down, stepped_norm, state_new_gate, state_new_up, state_new_down, state_new_norm)
```

```python
import functools

import jax
import jax.numpy as jnp
from jax import lax
from jax.experimental import pallas as pl
from jax.experimental.pallas import tpu as pltpu
from jax.sharding import PartitionSpec as P

MESH = pl.DeviceIdType.MESH
F32, BF16 = jnp.float32, jnp.bfloat16
learn_rate = 0.5
hold_rate = 0.9

Z = 8
X = 4
ROWS = 64
COLS = 768
HALF = 384
STEP = (1, -1)
LONG = ((3, 4), (4, 3))
SCALE = 8192.0


def encode(v):
    v = v * SCALE
    a = v * v
    a = a * a
    a = a * a
    return jnp.where(v < 0, -a, a).astype(BF16)


def decode(y):
    y = y.astype(F32)
    a = jnp.abs(y)
    q = lax.rsqrt(lax.rsqrt(jnp.maximum(a, 1e-37)))
    x = q * lax.rsqrt(q) * (1.0 / SCALE)
    x = jnp.where(a < 2e-37, 0.0, x)
    return jnp.where(y < 0, -x, x)


def plan():
    wire, lag = 1.06, 2.2
    tasks = {}
    for t in range(3):
        for d in range(2):
            for h in range(2):
                top = LONG[d][h]
                for k in range(top, 0, -1):
                    needs = [("got", "rs", t, d, h, k + 1)] if k < top else []
                    needs.append(("in", t, STEP[d] * k % Z))
                    tasks["rs", t, d, h, k] = (needs, 0.3 if k < top else 0.2, d, 100 + 10 * k - 3 * t)
                for k in range(1, top + 1):
                    needs = [("did", "update", t)] if k == 1 else []
                    if k > 1:
                        needs = [("got", "ag", t, d, h, k - 1)]
                    tasks["ag", t, d, h, k] = (needs, 0.05, d, 50 - 5 * k - t)
                tasks["ag", t, d, h, top + 1] = ([("got", "ag", t, d, h, top)], 0.05, None, 10)
        ends = [("got", "rs", t, d, h, 1) for d in range(2) for h in range(2)]
        tasks["sum", t] = (ends + [("in", t, 0)], 0.5, None, 200)
        tasks["master", t] = ([("late", 8.0 + t)], 0.3, None, 60)
        tasks["update", t] = ([("after", "sum", t, 3.0), ("did", "master", t)], 0.6, None, 190)
    tasks["norm_out",] = ([("did", "sum", 0)], 0.1, None, 55)
    tasks["norm_in",] = ([("after", "norm_out", 8.0)], 0.3, None, 54)
    order, now, free, arrive, done = [], 2.5, [0.0, 0.0], {}, {}

    def ready(needs):
        at = 0.0
        for n in needs:
            if n[0] == "got":
                at = max(at, arrive.get(n[1:], 1e9))
            elif n[0] == "in":
                off = (4, 3, 5, 2, 6, 1, 7, 0).index(n[2])
                at = max(at, 3.0 + 0.32 * (off * 3 + n[1] + 1))
            elif n[0] == "did":
                at = max(at, done.get(n[1:], 1e9))
            elif n[0] == "late":
                at = max(at, n[1])
            else:
                at = max(at, done.get(n[1:-1], 1e9) + n[-1])
        return at

    while tasks:
        times = {k: ready(v[0]) for k, v in tasks.items()}
        open_ = [k for k in tasks if times[k] <= now]
        if not open_:
            now = min(times.values())
            continue
        pick = max(open_, key=lambda k: (tasks[k][3], k))
        _, cost, link, _ = tasks.pop(pick)
        now += cost
        done[pick] = now
        order.append(pick)
        if link is not None:
            free[link] = max(free[link], now) + wire
            arrive[pick] = free[link] + lag
    return order, now


def kernel(*refs):
    it = iter(refs)
    take = lambda n: [next(it) for _ in range(n)]
    pg, pu, pd, pk, mg, mu, md, eg, eu, ed = take(10)
    cg, cu, cd, cn, sg, su, sd, tg, tu, td, own_n = take(11)
    own_gu, peer_gu, own_d, peer_d = take(4)
    rs_out_gu, rs_in_gu, rs_out_d, rs_in_d = take(4)
    ag_gu, ag_d = take(2)
    mean_gu, mean_d = take(2)
    mas_gu, mem_gu, mas_d, mem_d, mas_half, mem_half = take(6)
    new_gu, new_d, give_d = take(3)
    sq_gu, sq_d = take(2)
    packet, packets, norm_mas, norm_mem, cn_v, own_v = take(6)
    (load_sem, swap_s, swap_r, rs_s, rs_r, ag_s, ag_r, agp_s, agp_r, out_sem, mast_sem, half_s, half_r,
     sq_s, sq_r, pk_sem, pk_s, pk_r, new_sem, give_s, give_r, norm_sem) = take(22)

    r = lax.axis_index("replica")
    z, c = r // 2, r % 2
    peer = r + 1 - 2 * c
    x = lax.axis_index("model")
    chip = lambda off: lax.rem(z + off + 2 * Z, Z)
    beside = lambda d: {"replica": 2 * chip(STEP[d]) + c}
    across = lambda i: lax.rem(x + i, X)

    def remote(src, dst, s, rv, dev):
        return pltpu.make_async_remote_copy(src_ref=src, dst_ref=dst, send_sem=s, recv_sem=rv, device_id=dev, device_id_type=MESH)

    pending = []

    def go(copy):
        copy.start()
        pending.append(copy)
        return copy

    parts = (pg, pu, pd)

    def block(t, at, core):
        if t < 2:
            return parts[t].at[at, core]
        return pd.at[pl.ds(pl.multiple_of(HALF * core, HALF), HALF), pl.ds(pl.multiple_of(128 * at, 128), 128)]

    own_at = lambda t, at: own_gu.at[t, at] if t < 2 else own_d.at[at]
    peer_at = lambda t, at: peer_gu.at[t, at] if t < 2 else peer_d.at[at]
    offs = (4, 3, 5, 2, 6, 1, 7, 0)
    loads, swaps = {}, {}
    for off in offs:
        for t in range(3):
            at = chip(off)
            loads[t, off] = pltpu.make_async_copy(block(t, at, c), own_at(t, at), load_sem.at[t, off])
            loads[t, off].start()

    barrier = pltpu.get_barrier_semaphore()
    hello = [{"replica": peer}, beside(0), beside(1)]
    for i in range(1, X):
        hello.append({"model": across(i)})
        hello.append({"replica": peer, "model": across(i)})
    for dev in hello:
        pl.semaphore_signal(barrier, inc=1, device_id=dev, device_id_type=MESH)
    pl.semaphore_wait(barrier, len(hello))

    for off in offs:
        for t in range(3):
            at = chip(off)
            swaps[t, off] = remote(block(t, at, 1 - c), peer_at(t, at), swap_s.at[t, off], swap_r.at[t, off], {"replica": peer})
            swaps[t, off].start()

    masters = {}
    for t, (m, e) in enumerate(((mg, eg), (mu, eu), (md, ed))):
        for i, (ref, gu, dn) in enumerate(((m, mas_gu, mas_d), (e, mem_gu, mem_d))):
            masters[t, i] = pltpu.make_async_copy(ref, gu.at[t] if t < 2 else dn, mast_sem.at[t, i])
            masters[t, i].start()
    halves = []
    for i, (ref, buf) in enumerate(((md, mas_half), (ed, mem_half))):
        rows = pl.ds(pl.multiple_of(HALF * (1 - c), HALF), HALF)
        halves.append(remote(ref.at[rows], buf, half_s.at[i], half_r.at[i], {"replica": peer}))
        halves[-1].start()
    load_packet = pltpu.make_async_copy(pk, packet, pk_sem)
    load_packet.start()

    have = set()

    def need(t, off):
        if (t, off) not in have:
            have.add((t, off))
            loads[t, off].wait()
            swaps[t, off].wait_recv()
            pending_sends.append(swaps[t, off])

    pending_sends = []

    rs_out = lambda t, d, h, k: rs_out_gu.at[t, d, h, k - 1] if t < 2 else rs_out_d.at[d, h, k - 1]
    rs_in = lambda t, d, h, k: rs_in_gu.at[t, d, h, k - 1] if t < 2 else rs_in_d.at[d, h, k - 1]

    def rs_copy(t, d, h, k):
        return remote(rs_out(t, d, h, k), rs_in(t, d, h, k), rs_s.at[t, d, h, k - 1], rs_r.at[t, d, h, k - 1], beside(d))

    size = lambda t: 16 if t < 2 else 96

    def rs_send(t, d, h, k):
        off = STEP[d] * k % Z
        need(t, off)
        at, n = chip(off), size(t)
        chained = k < LONG[d][h]
        if chained:
            rs_copy(t, d, h, k + 1).wait_recv()
        own, other, out = own_at(t, at), peer_at(t, at), rs_out(t, d, h, k)
        arrived = rs_in(t, d, h, k + 1) if chained else None

        def body(i, _):
            here = pl.ds(pl.multiple_of(i * n, n), n)
            there = pl.ds(pl.multiple_of(2 * n * h + i * n, n), n)
            v = own[there, :] + other[there, :]
            if chained:
                v = v + decode(arrived[here, :])
            out[here, :] = encode(v)
            return 0

        lax.fori_loop(0, 2, body, 0)
        copy = rs_copy(t, d, h, k)
        copy.start()
        pending_sends.append(copy)

    def sq_slot(w, t):
        return sq_gu.at[w, t, x] if t < 2 else sq_d.at[w, 2 * x + c]

    def sq_copies(w, t):
        out = []
        for i in range(1, X):
            out.append(remote(sq_slot(w, t), sq_slot(w, t), sq_s.at[w, t, i], sq_r.at[w, t, i], {"model": across(i)}))
        if t == 2:
            for i in range(X):
                out.append(remote(sq_slot(w, t), sq_slot(w, t), sq_s.at[w, t, X + i], sq_r.at[w, t, X + i],
                                  {"replica": peer, "model": across(i)}))
        return out

    def share(w, t):
        for copy in sq_copies(w, t):
            copy.start()
            pending_sends.append(copy)

    def shared(w, t):
        for copy in sq_copies(w, t):
            copy.wait_recv()

    def lanes(v):
        total = v[:, :128]
        for j in range(1, v.shape[1] // 128):
            total = total + v[:, 128 * j : 128 * (j + 1)]
        return total

    def eights(v):
        total = v[:8]
        for j in range(1, v.shape[0] // 8):
            total = total + v[8 * j : 8 * (j + 1)]
        return total

    def sum_up(t):
        need(t, 0)
        for d in range(2):
            for h in range(2):
                rs_copy(t, d, h, 1).wait_recv()
        n = size(t)
        own, other = own_at(t, z), peer_at(t, z)
        for h in range(2):
            ahead, back = rs_in(t, 0, h, 1), rs_in(t, 1, h, 1)

            def body(i, carry):
                here = pl.ds(pl.multiple_of(i * n, n), n)
                there = pl.ds(pl.multiple_of(2 * n * h + i * n, n), n)
                v = (own[there, :] + other[there, :]) + (decode(ahead[here, :]) + decode(back[here, :]))
                v = v * (2 * Z) ** -0.5
                if t < 2:
                    mean_gu[t, there, :] = v
                    sq_gu[0, t, x, there, :] = lanes(v * v)
                    return carry
                mean_d[there, :] = v
                return carry + eights(v * v)

            first = jnp.zeros((8, 128), F32) if h == 0 else total
            total = lax.fori_loop(0, 2, body, first)
        if t == 2:
            sq_d[0, 2 * x + c] = total
        share(0, t)

    lane = lax.broadcasted_iota(jnp.int32, (96, 128), 1)
    mine = lax.broadcast_in_dim(c, (96, 128), ()) == jnp.where(lane < 64, 0, 1)

    def join(own, other):
        a = jnp.concatenate([own, own], axis=1)
        b = jnp.concatenate([other, other], axis=1)
        return jnp.where(mine, a, b)

    def master(t):
        masters[t, 0].wait()
        masters[t, 1].wait()
        n = size(t)
        if t == 2:
            halves[0].wait_recv()
            halves[1].wait_recv()
            pending_sends.extend(halves)

        def body(i, carry):
            here = pl.ds(pl.multiple_of(i * n, n), n)
            if t < 2:
                v = mas_gu[t, here, :]
                sq_gu[1, t, x, here, :] = lanes(v * v)
                return carry
            there = pl.ds(pl.multiple_of(HALF * c + i * n, n), n)
            v = join(mas_d[there, :], mas_half[here, :])
            return carry + eights(v * v)

        total = lax.fori_loop(0, 4, body, jnp.zeros((8, 128), F32))
        if t == 2:
            sq_d[1, 2 * x + c] = total
        share(1, t)

    def update(t):
        shared(0, t)
        shared(1, t)
        n = size(t)
        if t == 2:
            def ratio_of(w):
                total = sq_d[w, 0]
                for j in range(1, 2 * X):
                    total = total + sq_d[w, j]
                return jnp.sum(total, axis=0, keepdims=True)
            ratio_d = jnp.sqrt(ratio_of(1)) * lax.rsqrt(ratio_of(0) + 1e-6)

        def body(i, _):
            here = pl.ds(pl.multiple_of(i * n, n), n)
            if t < 2:
                def whole(w):
                    total = sq_gu[w, t, 0, here, :]
                    for j in range(1, X):
                        total = total + sq_gu[w, t, j, here, :]
                    return jnp.sum(total, axis=1, keepdims=True)
                ratio = jnp.sqrt(whole(1)) * lax.rsqrt(whole(0) + 1e-6)
                state = hold_rate * mem_gu[t, here, :] + mean_gu[t, here, :] * ratio
                stepped = mas_gu[t, here, :] - learn_rate * state
                new_gu[t, 0, here, :] = stepped
                new_gu[t, 1, here, :] = state
                ag_gu[t, z, here, :] = stepped.astype(BF16)
                return 0
            there = pl.ds(pl.multiple_of(HALF * c + i * n, n), n)
            state = hold_rate * join(mem_d[there, :], mem_half[here, :]) + mean_d[here, :] * ratio_d
            stepped = join(mas_d[there, :], mas_half[here, :]) - learn_rate * state
            ag_d[z, here, :] = stepped.astype(BF16)
            for j, v in enumerate((stepped, state)):
                turned = jnp.concatenate([v[:, 64:], v[:, :64]], axis=1)
                new_d[j, here, :] = jnp.where(mine[:, :64], v[:, :64], turned[:, :64])
                give_d[j, here, :] = jnp.where(mine[:, :64], turned[:, :64], v[:, :64])
            return 0

        lax.fori_loop(0, 4, body, 0)
        if t < 2:
            for j, ref in enumerate(((sg, su)[t], (tg, tu)[t])):
                go(pltpu.make_async_copy(new_gu.at[t, j], ref, new_sem.at[t, j]))
        else:
            rows = pl.ds(pl.multiple_of(HALF * c, HALF), HALF)
            for j, ref in enumerate((sd, td)):
                go(pltpu.make_async_copy(new_d.at[j], ref.at[rows], new_sem.at[t, j]))
                gift = remote(give_d.at[j], ref.at[rows], give_s.at[j], give_r.at[j], {"replica": peer})
                gift.start()
                gifts.append(gift)
        for h in range(2):
            deliver(t, 0, h)

    gifts = []
    ag_at = lambda t, at, h: ag_gu.at[t, at, pl.ds(32 * h, 32)] if t < 2 else ag_d.at[at, pl.ds(192 * h, 192)]

    def place(t, at, h, core):
        if t < 2:
            return (cg, cu)[t].at[at, core, pl.ds(32 * h, 32)]
        return cd.at[pl.ds(pl.multiple_of(HALF * core + 192 * h, 192), 192), pl.ds(pl.multiple_of(128 * at, 128), 128)]

    delivered = []

    def deliver(t, off, h):
        at = chip(off)
        go(pltpu.make_async_copy(ag_at(t, at, h), place(t, at, h, c), out_sem.at[t, off % Z, h]))
        copy = remote(ag_at(t, at, h), place(t, at, h, c), agp_s.at[t, off % Z, h], agp_r.at[t, off % Z, h], {"replica": peer})
        copy.start()
        delivered.append(copy)

    def ag_copy(t, d, h, k, from_here):
        at = chip(-STEP[d] * (k - 1)) if from_here else chip(-STEP[d] * k)
        return remote(ag_at(t, at, h), ag_at(t, at, h), ag_s.at[t, d, h, k - 1], ag_r.at[t, d, h, k - 1], beside(d))

    def ag_step(t, d, h, k):
        if k > 1:
            ag_copy(t, d, h, k - 1, False).wait_recv()
        if k <= LONG[d][h]:
            copy = ag_copy(t, d, h, k, True)
            copy.start()
            pending_sends.append(copy)
        if k > 1:
            deliver(t, -STEP[d] * (k - 1), h)

    def norm_copies():
        return [remote(packet, packets.at[r], pk_s.at[j], pk_r.at[j], {"replica": lax.rem(r + j, 2 * Z)}) for j in range(1, 2 * Z)]

    def norm_out():
        load_packet.wait()
        for copy in norm_copies():
            copy.start()
            pending_sends.append(copy)

    def norm_in():
        packets[r] = packet[...]
        for copy in norm_copies():
            copy.wait_recv()
        total = packets[0, :8, :]
        for j in range(1, 2 * Z):
            total = total + packets[j, :8, :]
        mean = total * (2 * Z) ** -0.5
        low = lax.broadcasted_iota(jnp.int32, (1, 128), 1) < 64
        turn = lambda v: jnp.concatenate([v[:, 64:], v[:, :64]], axis=1)
        for j in range(Z):
            a, b = packets[2 * j, 8:9, :], packets[2 * j + 1, 8:9, :]
            norm_mas[j : j + 1, :] = jnp.where(low, a, turn(b))
            norm_mem[j : j + 1, :] = jnp.where(low, turn(a), b)
        state = hold_rate * norm_mem[...] + mean
        stepped = norm_mas[...] - learn_rate * state
        cn_v[...] = stepped.astype(BF16)
        row = lax.broadcasted_iota(jnp.int32, (8, 128), 0) == z
        pick = lambda v: jnp.sum(jnp.where(row, v, 0.0), axis=0, keepdims=True)
        a, b = pick(stepped), pick(state)
        core0 = lax.broadcast_in_dim(c, (1, 128), ()) == 0
        own_v[...] = jnp.where(low, jnp.where(core0, a, turn(a)), jnp.where(core0, turn(b), b))
        go(pltpu.make_async_copy(cn_v, cn, norm_sem.at[0]))
        go(pltpu.make_async_copy(own_v, own_n, norm_sem.at[1]))

    acts = {"rs": rs_send, "ag": ag_step, "sum": sum_up, "master": master, "update": update, "norm_out": norm_out, "norm_in": norm_in}
    for name, *args in plan()[0]:
        acts[name](*args)

    for copy in delivered + gifts:
        copy.wait_recv()
        copy.wait_send()
    for copy in pending_sends:
        copy.wait_send()
    for copy in pending:
        copy.wait()


def call(pg, pu, pd, pk, mg, mu, md, eg, eu, ed):
    S = jax.ShapeDtypeStruct
    dma = pltpu.SemaphoreType.DMA
    outs = (
        S((Z, 2, ROWS, COLS), BF16), S((Z, 2, ROWS, COLS), BF16), S((2 * HALF, 128 * Z), BF16), S((8, 128), BF16),
        S((ROWS, COLS), F32), S((ROWS, COLS), F32), S((2 * HALF, 64), F32),
        S((ROWS, COLS), F32), S((ROWS, COLS), F32), S((2 * HALF, 64), F32), S((1, 128), F32),
    )
    v = pltpu.VMEM
    scratch = [
        v((2, Z, ROWS, COLS), F32), v((2, Z, ROWS, COLS), F32), v((Z, HALF, 128), F32), v((Z, HALF, 128), F32),
        v((2, 2, 2, 4, 32, COLS), BF16), v((2, 2, 2, 4, 32, COLS), BF16), v((2, 2, 4, 192, 128), BF16), v((2, 2, 4, 192, 128), BF16),
        v((2, Z, ROWS, COLS), BF16), v((Z, HALF, 128), BF16),
        v((2, ROWS, COLS), F32), v((HALF, 128), F32),
        v((2, ROWS, COLS), F32), v((2, ROWS, COLS), F32), v((2 * HALF, 64), F32), v((2 * HALF, 64), F32), v((HALF, 64), F32), v((HALF, 64), F32),
        v((2, 2, ROWS, COLS), F32), v((2, HALF, 64), F32), v((2, HALF, 64), F32),
        v((2, 2, X, ROWS, 128), F32), v((2, 2 * X, 8, 128), F32),
        v((16, 128), F32), v((2 * Z, 16, 128), F32), v((8, 128), F32), v((8, 128), F32), v((8, 128), BF16), v((1, 128), F32),
        dma((3, Z)), dma((3, Z)), dma((3, Z)), dma((3, 2, 2, 4)), dma((3, 2, 2, 4)), dma((3, 2, 2, 4)), dma((3, 2, 2, 4)),
        dma((3, Z, 2)), dma((3, Z, 2)), dma((3, Z, 2)), dma((3, 2)), dma((2,)), dma((2,)),
        dma((2, 3, 2 * X)), dma((2, 3, 2 * X)), dma(()), dma((2 * Z,)), dma((2 * Z,)), dma((3, 2)), dma((2,)), dma((2,)), dma((2,)),
    ]
    any_ = pl.BlockSpec(memory_space=pl.ANY)
    return pl.pallas_call(
        kernel,
        out_shape=outs,
        in_specs=[any_] * 10,
        out_specs=[any_] * len(outs),
        scratch_shapes=scratch,
        compiler_params=pltpu.CompilerParams(collective_id=0, has_side_effects=True, vmem_limit_bytes=48 * 2**20),
    )(pg, pu, pd, pk, mg, mu, md, eg, eu, ed)


def on_device(pg, pu, pd, pn, mg, mu, md, mn, eg, eu, ed, en):
    pk = jnp.concatenate([pn[0], mn, en, jnp.zeros((896,), F32)]).reshape(16, 128)
    cg, cu, cd, cn, sg, su, sd, tg, tu, td, own = call(
        pg.reshape(Z, 2, ROWS, COLS), pu.reshape(Z, 2, ROWS, COLS), pd[0], pk, mg, mu, md, eg, eu, ed
    )
    flat = (2 * Z * ROWS, COLS)
    return (cg.reshape(flat), cu.reshape(flat), cd, cn.reshape(-1), sg, su, sd, own[0, :64], tg, tu, td, own[0, 64:])


def solution(mesh):
    rows, cols = P(("shift", "replica"), "model"), P(("shift", "model"), "replica")
    vec = P(("shift", "replica"))
    return jax.shard_map(
        on_device,
        mesh=mesh,
        in_specs=(
            P(("shift", "replica"), None, "model"), P(("shift", "replica"), None, "model"), P(("shift", "replica"), "model", None),
            P(("shift", "replica"), None), rows, rows, cols, vec, rows, rows, cols, vec,
        ),
        out_specs=(
            P("shift", "model"), P("shift", "model"), P(("shift", "model"), None), P("shift"),
            rows, rows, cols, vec, rows, rows, cols, vec,
        ),
        check_vma=False,
    )
```

```python
import functools

import jax
import jax.numpy as jnp
from jax import lax
from jax.experimental import pallas as pl
from jax.experimental.pallas import tpu as pltpu
from jax.sharding import PartitionSpec as P

MESH = pl.DeviceIdType.MESH
F32, BF16 = jnp.float32, jnp.bfloat16
learn_rate = 0.5
hold_rate = 0.9

Z = 8
X = 4
ROWS = 64
COLS = 768
HALF = 384
STEP = (1, -1)
LONG = ((3, 4), (4, 3))
SCALE = 8192.0


def encode(v):
    v = v * SCALE
    a = v * v
    a = a * a
    a = a * a
    return jnp.where(v < 0, -a, a).astype(BF16)


def decode(y):
    y = y.astype(F32)
    a = jnp.abs(y)
    q = lax.rsqrt(lax.rsqrt(jnp.maximum(a, 1e-37)))
    x = q * lax.rsqrt(q) * (1.0 / SCALE)
    x = jnp.where(a < 2e-37, 0.0, x)
    return jnp.where(y < 0, -x, x)


def plan():
    wire, lag = 1.06, 2.2
    tasks = {}
    for t in range(3):
        for d in range(2):
            for h in range(2):
                top = LONG[d][h]
                for k in range(top, 0, -1):
                    needs = [("got", "rs", t, d, h, k + 1)] if k < top else []
                    needs.append(("in", t, STEP[d] * k % Z))
                    tasks["rs", t, d, h, k] = (needs, 0.3 if k < top else 0.2, d, 100 + 10 * k - 3 * t)
                for k in range(2, top + 1):
                    tasks["ag", t, d, h, k] = ([("got", "ag", t, d, h, k - 1)], 0.05, d, 50 - 5 * k - t)
                tasks["ag", t, d, h, top + 1] = ([("got", "ag", t, d, h, top)], 0.05, None, 10)
        ends = [("got", "rs", t, d, h, 1) for d in range(2) for h in range(2)]
        tasks["sum", t] = (ends + [("in", t, 0)], 0.5, None, 200)
        tasks["master", t] = ([("late", 8.0 + t)], 0.3, None, 60)
        tasks["update", t] = ([("after", "sum", t, 3.0), ("did", "master", t)], 0.6, None, 190)
    tasks["norm_out",] = ([("did", "sum", 0)], 0.1, None, 55)
    tasks["norm_in",] = ([("after", "norm_out", 8.0)], 0.3, None, 54)
    order, now, free, arrive, done = [], 2.5, [0.0, 0.0], {}, {}

    def ready(needs):
        at = 0.0
        for n in needs:
            if n[0] == "got":
                at = max(at, arrive.get(n[1:], 1e9))
            elif n[0] == "in":
                off = (4, 3, 5, 2, 6, 1, 7, 0).index(n[2])
                at = max(at, 3.0 + 0.32 * (off * 3 + n[1] + 1))
            elif n[0] == "did":
                at = max(at, done.get(n[1:], 1e9))
            elif n[0] == "late":
                at = max(at, n[1])
            else:
                at = max(at, done.get(n[1:-1], 1e9) + n[-1])
        return at

    while tasks:
        times = {k: ready(v[0]) for k, v in tasks.items()}
        open_ = [k for k in tasks if times[k] <= now]
        if not open_:
            now = min(times.values())
            continue
        pick = max(open_, key=lambda k: (tasks[k][3], k))
        _, cost, link, _ = tasks.pop(pick)
        now += cost
        done[pick] = now
        order.append(pick)
        sent = [(pick, link)] if link is not None else []
        if pick[0] == "update":
            sent = [(("ag", pick[1], d, h, 1), d) for h in range(2) for d in range(2)]
        for name, link in sent:
            free[link] = max(free[link], now) + wire
            arrive[name] = free[link] + lag
    return order, now


def kernel(*refs):
    it = iter(refs)
    take = lambda n: [next(it) for _ in range(n)]
    pg, pu, pd, pn, mg, mu, md, mn, eg, eu, ed, en = take(12)
    cg, cu, cd, cn, sg, su, sd, sn, tg, tu, td, tn = take(12)
    own_gu, peer_gu, own_d, peer_d = take(4)
    rs_out_gu, rs_in_gu, rs_out_d, rs_in_d = take(4)
    mean_gu, mean_d = take(2)
    mas_gu, mem_gu, mas_d, mem_d = take(4)
    give_d = take(1)[0]
    sq_gu, sq_d = take(2)
    packet, packets, norm_mas, norm_mem, mn_v, en_v = take(6)
    (load_sem, swap_s, swap_r, rs_s, rs_r, ag_s, ag_r, agp_s, agp_r, mast_sem, half_s, half_r,
     sq_s, sq_r, pk_sem, pk_s, pk_r, give_s, give_r) = take(19)

    r = lax.axis_index("replica")
    z, c = r // 2, r % 2
    peer = r + 1 - 2 * c
    x = lax.axis_index("model")
    chip = lambda off: lax.rem(z + off + 2 * Z, Z)
    beside = lambda d: {"replica": 2 * chip(STEP[d]) + c}
    across = lambda i: lax.rem(x + i, X)

    def remote(src, dst, s, rv, dev):
        return pltpu.make_async_remote_copy(src_ref=src, dst_ref=dst, send_sem=s, recv_sem=rv, device_id=dev, device_id_type=MESH)

    parts = (pg, pu, pd)

    def block(t, at, core):
        if t < 2:
            return parts[t].at[at, core]
        return pd.at[pl.ds(pl.multiple_of(HALF * core, HALF), HALF), pl.ds(pl.multiple_of(128 * at, 128), 128)]

    own_at = lambda t, at: own_gu.at[t, at] if t < 2 else own_d.at[at]
    peer_at = lambda t, at: peer_gu.at[t, at] if t < 2 else peer_d.at[at]
    offs = (4, 3, 5, 2, 6, 1, 7, 0)
    loads, swaps = {}, {}
    for off in offs:
        for t in range(3):
            at = chip(off)
            loads[t, off] = pltpu.make_async_copy(block(t, at, c), own_at(t, at), load_sem.at[t, off])
            loads[t, off].start()

    barrier = pltpu.get_barrier_semaphore()
    hello = [{"replica": peer}, beside(0), beside(1)]
    for i in range(1, X):
        hello.append({"model": across(i)})
        hello.append({"replica": peer, "model": across(i)})
    for dev in hello:
        pl.semaphore_signal(barrier, inc=1, device_id=dev, device_id_type=MESH)
    pl.semaphore_wait(barrier, len(hello))

    for off in offs:
        for t in range(3):
            at = chip(off)
            swaps[t, off] = remote(block(t, at, 1 - c), peer_at(t, at), swap_s.at[t, off], swap_r.at[t, off], {"replica": peer})
            swaps[t, off].start()

    masters = {}
    halves = []
    half = lambda core: pl.ds(pl.multiple_of(HALF * core, HALF), HALF)
    mine, theirs = pl.ds(pl.multiple_of(64 * c, 64), 64), pl.ds(pl.multiple_of(64 * (1 - c), 64), 64)
    for t, pair in enumerate(((mg, eg), (mu, eu), (md, ed))):
        for i, ref in enumerate(pair):
            if t < 2:
                src, dst = ref, (mas_gu, mem_gu)[i].at[t]
            else:
                src, dst = ref.at[:, half(c)], (mas_d, mem_d)[i].at[mine]
                halves.append(remote(ref.at[:, half(1 - c)], dst, half_s.at[i], half_r.at[i], {"replica": peer}))
                halves[-1].start()
            masters[t, i] = pltpu.make_async_copy(src, dst, mast_sem.at[t, i])
            masters[t, i].start()
    load_packet = [
        pltpu.make_async_copy(ref, dst, pk_sem.at[j]) for j, (ref, dst) in enumerate(((pn, packet.at[:8]), (mn, mn_v), (en, en_v)))
    ]
    for copy in load_packet:
        copy.start()

    have = set()

    def need(t, off):
        if (t, off) not in have:
            have.add((t, off))
            loads[t, off].wait()
            swaps[t, off].wait_recv()
            pending_sends.append(swaps[t, off])

    pending_sends = []

    rs_out = lambda t, d, h, k: rs_out_gu.at[t, d, h, k - 1] if t < 2 else rs_out_d.at[d, h, k - 1]
    rs_in = lambda t, d, h, k: rs_in_gu.at[t, d, h, k - 1] if t < 2 else rs_in_d.at[d, h, k - 1]

    def rs_copy(t, d, h, k):
        return remote(rs_out(t, d, h, k), rs_in(t, d, h, k), rs_s.at[t, d, h, k - 1], rs_r.at[t, d, h, k - 1], beside(d))

    size = lambda t: 16 if t < 2 else 96

    def rs_send(t, d, h, k):
        off = STEP[d] * k % Z
        need(t, off)
        at, n = chip(off), size(t)
        chained = k < LONG[d][h]
        if chained:
            rs_copy(t, d, h, k + 1).wait_recv()
        own, other, out = own_at(t, at), peer_at(t, at), rs_out(t, d, h, k)
        arrived = rs_in(t, d, h, k + 1) if chained else None

        def body(i, _):
            here = pl.ds(pl.multiple_of(i * n, n), n)
            there = pl.ds(pl.multiple_of(2 * n * h + i * n, n), n)
            v = own[there, :] + other[there, :]
            if chained:
                v = v + decode(arrived[here, :])
            out[here, :] = encode(v)
            return 0

        lax.fori_loop(0, 2, body, 0)
        copy = rs_copy(t, d, h, k)
        copy.start()
        pending_sends.append(copy)

    def sq_slot(w, t):
        return sq_gu.at[w, t, x] if t < 2 else sq_d.at[w, 2 * x + c]

    def sq_copies(w, t):
        out = []
        for i in range(1, X):
            out.append(remote(sq_slot(w, t), sq_slot(w, t), sq_s.at[w, t, i], sq_r.at[w, t, i], {"model": across(i)}))
        if t == 2:
            for i in range(X):
                out.append(remote(sq_slot(w, t), sq_slot(w, t), sq_s.at[w, t, X + i], sq_r.at[w, t, X + i],
                                  {"replica": peer, "model": across(i)}))
        return out

    def share(w, t):
        for copy in sq_copies(w, t):
            copy.start()
            pending_sends.append(copy)

    def shared(w, t):
        for copy in sq_copies(w, t):
            copy.wait_recv()

    def lanes(v):
        total = v[:, :128]
        for j in range(1, v.shape[1] // 128):
            total = total + v[:, 128 * j : 128 * (j + 1)]
        return total

    def eights(v):
        total = v[:8]
        for j in range(1, v.shape[0] // 8):
            total = total + v[8 * j : 8 * (j + 1)]
        return total

    def sum_up(t):
        need(t, 0)
        for d in range(2):
            for h in range(2):
                rs_copy(t, d, h, 1).wait_recv()
        n = size(t)
        own, other = own_at(t, z), peer_at(t, z)
        for h in range(2):
            ahead, back = rs_in(t, 0, h, 1), rs_in(t, 1, h, 1)

            def body(i, carry):
                here = pl.ds(pl.multiple_of(i * n, n), n)
                there = pl.ds(pl.multiple_of(2 * n * h + i * n, n), n)
                v = (own[there, :] + other[there, :]) + (decode(ahead[here, :]) + decode(back[here, :]))
                v = v * (2 * Z) ** -0.5
                if t < 2:
                    mean_gu[t, there, :] = v
                    sq_gu[0, t, x, there, :] = lanes(v * v)
                    return carry
                mean_d[there, :] = v
                return carry + eights(v * v)

            first = jnp.zeros((8, 128), F32) if h == 0 else total
            total = lax.fori_loop(0, 2, body, first)
        if t == 2:
            sq_d[0, 2 * x + c] = total
        share(0, t)

    def master(t):
        masters[t, 0].wait()
        masters[t, 1].wait()
        if t < 2:

            def body(i, _):
                here = pl.ds(pl.multiple_of(16 * i, 16), 16)
                v = mas_gu[t, here, :]
                sq_gu[1, t, x, here, :] = lanes(v * v)
                return 0

            lax.fori_loop(0, 4, body, 0)
        else:
            halves[0].wait_recv()
            halves[1].wait_recv()
            pending_sends.extend(halves)

            def body(i, carry):
                v = mas_d[:, pl.ds(pl.multiple_of(128 * i, 128), 128)]
                return carry + v * v

            total = lax.fori_loop(0, HALF // 128, body, jnp.zeros((128, 128), F32))
            sq_d[1, 2 * x + c] = eights(total.T)
        share(1, t)

    def update(t):
        shared(0, t)
        shared(1, t)
        if t < 2:

            def body(i, _):
                here = pl.ds(pl.multiple_of(16 * i, 16), 16)

                def whole(w):
                    total = sq_gu[w, t, 0, here, :]
                    for j in range(1, X):
                        total = total + sq_gu[w, t, j, here, :]
                    return jnp.sum(total, axis=1, keepdims=True)

                ratio = jnp.sqrt(whole(1)) * lax.rsqrt(whole(0) + 1e-6)
                state = hold_rate * mem_gu[t, here, :] + mean_gu[t, here, :] * ratio
                stepped = mas_gu[t, here, :] - learn_rate * state
                (sg, su)[t][here, :] = stepped
                (tg, tu)[t][here, :] = state
                (cg, cu)[t][z, c, here, :] = stepped.astype(BF16)
                return 0

            lax.fori_loop(0, 4, body, 0)
        else:

            def whole(w):
                total = sq_d[w, 0]
                for j in range(1, 2 * X):
                    total = total + sq_d[w, j]
                return jnp.sum(total, axis=0, keepdims=True)

            ratio = jnp.sqrt(whole(1)) * lax.rsqrt(whole(0) + 1e-6)

            def body(i, _):
                here = pl.ds(pl.multiple_of(128 * i, 128), 128)
                state = hold_rate * mem_d[:, here] + (mean_d[here, :] * ratio).T
                stepped = mas_d[:, here] - learn_rate * state
                cd[z, c, here, :] = stepped.T.astype(BF16)
                there = pl.ds(pl.multiple_of(HALF * c + 128 * i, 128), 128)
                for j, v in enumerate((stepped, state)):
                    (sd, td)[j][:, there] = jnp.where(low_core, v[:64], v[64:])
                    give_d[j, :, here] = jnp.where(low_core, v[64:], v[:64])
                return 0

            low_core = lax.broadcast_in_dim(c, (64, 128), ()) == 0
            lax.fori_loop(0, HALF // 128, body, 0)
        for h in range(2):
            for d in range(2):
                ag_step(t, d, h, 1)
        for h in range(2):
            deliver(t, 0, h)
        if t == 2:
            for j, ref in enumerate((sd, td)):
                gift = remote(give_d.at[j], ref.at[:, half(c)], give_s.at[j], give_r.at[j], {"replica": peer})
                gift.start()
                gifts.append(gift)

    gifts = []

    def ag_at(t, at, h):
        return (cg, cu, cd)[t].at[at, c, pl.ds((32, 32, 192)[t] * h, (32, 32, 192)[t])]

    delivered = []

    def deliver(t, off, h):
        at = chip(off)
        copy = remote(ag_at(t, at, h), ag_at(t, at, h), agp_s.at[t, off % Z, h], agp_r.at[t, off % Z, h], {"replica": peer})
        copy.start()
        delivered.append(copy)

    def ag_copy(t, d, h, k, from_here):
        at = chip(-STEP[d] * (k - 1)) if from_here else chip(-STEP[d] * k)
        return remote(ag_at(t, at, h), ag_at(t, at, h), ag_s.at[t, d, h, k - 1], ag_r.at[t, d, h, k - 1], beside(d))

    def ag_step(t, d, h, k):
        if k > 1:
            ag_copy(t, d, h, k - 1, False).wait_recv()
        if k <= LONG[d][h]:
            copy = ag_copy(t, d, h, k, True)
            copy.start()
            pending_sends.append(copy)
        if k > 1:
            deliver(t, -STEP[d] * (k - 1), h)

    def norm_copies():
        return [remote(packet, packets.at[r], pk_s.at[j], pk_r.at[j], {"replica": lax.rem(r + j, 2 * Z)}) for j in range(1, 2 * Z)]

    turn = lambda v: jnp.concatenate([v[:, 64:], v[:, :64]], axis=1)

    def norm_out():
        for copy in load_packet:
            copy.wait()
        packet[8:9, :] = jnp.concatenate([mn_v[...], en_v[...]], axis=1)
        for copy in norm_copies():
            copy.start()
            pending_sends.append(copy)

    def norm_in():
        packets[r] = packet[...]
        for copy in norm_copies():
            copy.wait_recv()
        total = packets[0, :8, :]
        for j in range(1, 2 * Z):
            total = total + packets[j, :8, :]
        mean = total * (2 * Z) ** -0.5
        low = lax.broadcasted_iota(jnp.int32, (1, 128), 1) < 64
        for j in range(Z):
            a, b = packets[2 * j, 8:9, :], packets[2 * j + 1, 8:9, :]
            norm_mas[j : j + 1, :] = jnp.where(low, a, turn(b))
            norm_mem[j : j + 1, :] = jnp.where(low, turn(a), b)
        state = hold_rate * norm_mem[...] + mean
        stepped = norm_mas[...] - learn_rate * state
        cn[...] = stepped.astype(BF16)
        row = lax.broadcasted_iota(jnp.int32, (8, 128), 0) == z
        pick = lambda v: jnp.sum(jnp.where(row, v, 0.0), axis=0, keepdims=True)
        a, b = pick(stepped), pick(state)
        first = lax.broadcast_in_dim(c, (1, 64), ()) == 0
        sn[...] = jnp.where(first, a[:, :64], turn(a)[:, :64])
        tn[...] = jnp.where(first, b[:, :64], turn(b)[:, :64])

    acts = {"rs": rs_send, "ag": ag_step, "sum": sum_up, "master": master, "update": update, "norm_out": norm_out, "norm_in": norm_in}
    for name, *args in plan()[0]:
        acts[name](*args)

    for copy in delivered + gifts:
        copy.wait_recv()
    for copy in pending_sends + delivered + gifts:
        copy.wait_send()


def write(*refs):
    src, dst, sem = refs[:12], refs[12:24], refs[24]
    copies = []

    def put(a, b):
        copies.append(pltpu.make_async_copy(a, b, sem.at[len(copies)]))
        copies[-1].start()

    for i in range(12):
        if i != 2:
            put(src[i], dst[i])
            continue
        for at in range(Z):
            for core in range(2):
                put(src[i].at[at, core], dst[i].at[pl.ds(HALF * core, HALF), pl.ds(128 * at, 128)])
    for copy in copies:
        copy.wait()


def call(*args):
    S = jax.ShapeDtypeStruct
    dma = pltpu.SemaphoreType.DMA
    outs = (
        S((Z, 2, ROWS, COLS), BF16), S((Z, 2, ROWS, COLS), BF16), S((Z, 2, HALF, 128), BF16), S((8, 128), BF16),
        S((ROWS, COLS), F32), S((ROWS, COLS), F32), S((64, 2 * HALF), F32), S((1, 64), F32),
        S((ROWS, COLS), F32), S((ROWS, COLS), F32), S((64, 2 * HALF), F32), S((1, 64), F32),
    )
    v = pltpu.VMEM
    scratch = [
        v((2, Z, ROWS, COLS), F32), v((2, Z, ROWS, COLS), F32), v((Z, HALF, 128), F32), v((Z, HALF, 128), F32),
        v((2, 2, 2, 4, 32, COLS), BF16), v((2, 2, 2, 4, 32, COLS), BF16), v((2, 2, 4, 192, 128), BF16), v((2, 2, 4, 192, 128), BF16),
        v((2, ROWS, COLS), F32), v((HALF, 128), F32),
        v((2, ROWS, COLS), F32), v((2, ROWS, COLS), F32), v((128, HALF), F32), v((128, HALF), F32),
        v((2, 64, HALF), F32),
        v((2, 2, X, ROWS, 128), F32), v((2, 2 * X, 8, 128), F32),
        v((16, 128), F32), v((2 * Z, 16, 128), F32), v((8, 128), F32), v((8, 128), F32), v((1, 64), F32), v((1, 64), F32),
        dma((3, Z)), dma((3, Z)), dma((3, Z)), dma((3, 2, 2, 4)), dma((3, 2, 2, 4)), dma((3, 2, 2, 4)), dma((3, 2, 2, 4)),
        dma((3, Z, 2)), dma((3, Z, 2)), dma((3, 2)), dma((2,)), dma((2,)),
        dma((2, 3, 2 * X)), dma((2, 3, 2 * X)), dma((3,)), dma((2 * Z,)), dma((2 * Z,)), dma((2,)), dma((2,)),
    ]
    any_, hbm = pl.BlockSpec(memory_space=pl.ANY), pl.BlockSpec(memory_space=pltpu.HBM)
    args = [pltpu.with_memory_space_constraint(a, pltpu.HBM) for a in args]
    results = pl.pallas_call(
        kernel,
        out_shape=outs,
        in_specs=[hbm] * len(args),
        out_specs=[pl.BlockSpec(memory_space=pltpu.VMEM)] * len(outs),
        scratch_shapes=scratch,
        compiler_params=pltpu.CompilerParams(collective_id=0, has_side_effects=True, vmem_limit_bytes=28 * 2**20),
    )(*args)
    return pl.pallas_call(
        write,
        out_shape=outs[:2] + (S((2 * HALF, 128 * Z), BF16),) + outs[3:],
        in_specs=[any_] * len(outs),
        out_specs=[hbm] * len(outs),
        scratch_shapes=[dma((2 * Z + 11,))],
        compiler_params=pltpu.CompilerParams(vmem_limit_bytes=2**20),
    )(*results)


def on_device(pg, pu, pd, pn, mg, mu, md, mn, eg, eu, ed, en):
    wide = lambda p: p.reshape(Z, 2, ROWS, COLS)
    cg, cu, cd, cn, sg, su, sd, sn, tg, tu, td, tn = call(
        wide(pg), wide(pu), pd[0], pn.reshape(8, 128), mg, mu, md.T, mn.reshape(1, -1), eg, eu, ed.T, en.reshape(1, -1)
    )
    flat = (2 * Z * ROWS, COLS)
    return (cg.reshape(flat), cu.reshape(flat), cd, cn.reshape(-1), sg, su, sd.T, sn[0], tg, tu, td.T, tn[0])


def solution(mesh):
    rows, cols = P(("shift", "replica"), "model"), P(("shift", "model"), "replica")
    vec = P(("shift", "replica"))
    return jax.shard_map(
        on_device,
        mesh=mesh,
        in_specs=(
            P(("shift", "replica"), None, "model"), P(("shift", "replica"), None, "model"), P(("shift", "replica"), "model", None),
            P(("shift", "replica"), None), rows, rows, cols, vec, rows, rows, cols, vec,
        ),
        out_specs=(
            P("shift", "model"), P("shift", "model"), P(("shift", "model"), None), P("shift"),
            rows, rows, cols, vec, rows, rows, cols, vec,
        ),
        check_vma=False,
    )
```

```python
import functools

import jax
import jax.numpy as jnp
from jax import lax
from jax.experimental import pallas as pl
from jax.experimental.pallas import tpu as pltpu
from jax.sharding import PartitionSpec as P

MESH = pl.DeviceIdType.MESH
F32, BF16 = jnp.float32, jnp.bfloat16
learn_rate = 0.5
hold_rate = 0.9

Z = 8
X = 4
ROWS = 64
COLS = 768
HALF = 384
STEP = (1, -1)
SCALE = 8192.0


AHEAD = 3


def encode(v):
    v = v * SCALE
    a = v * v
    a = a * a
    a = a * a
    return jnp.where(v < 0, -a, a).astype(BF16)


def decode(y):
    y = y.astype(F32)
    a = jnp.abs(y)
    q = lax.rsqrt(lax.rsqrt(jnp.maximum(a, 1e-37)))
    x = q * lax.rsqrt(q) * (1.0 / SCALE)
    x = jnp.where(a < 2e-37, 0.0, x)
    return jnp.where(y < 0, -x, x)


ORDER = (
    "r0L4", "r0S3", "r2L4", "r1L4", "r0L3", "r0S2", "m0", "r2L3", "r1L3", "m1", "r0L2", "r1S3", "m2", "r0S1", "r1L2",
    "r0L1", "r1S2", "r2S3", "r2L2", "s0", "n0", "r1L1", "r1S1", "r2S2", "r2L1", "u0", "s1", "r2S1", "a0L2", "a0S2", "n1",
    "u1", "s2", "a0L3", "a0S3", "a1L2", "u2", "a1S2", "a1L3", "a2L2", "a0L4", "a2S2", "a2L3", "a1L4", "a1S3",
    "a0L5", "a2S3", "a2L4", "a1L5", "n2", "a2S4", "a1S4", "a0S4", "a2L5",
)
TOP = {"L": 4, "S": 3}


def slot(p, k):
    return TOP[p] - k + (0 if p == "L" else 4)


def kernel(*refs):
    it = iter(refs)
    take = lambda n: [next(it) for _ in range(n)]
    pg, pu, pd, pn, mg, mu, md, mn, eg, eu, ed, en = take(12)
    cg, cu, cd, cn, sg, su, sd, sn, tg, tu, td, tn = take(12)
    own_gu, peer_gu, own_d, peer_d = take(4)
    rs_out_gu, rs_in_gu, rs_out_d, rs_in_d = take(4)
    mean_gu, mean_d = take(2)
    mas_gu, mem_gu, mas_d, mem_d = take(4)
    give_d = take(1)[0]
    sq_gu, sq_d = take(2)
    pn_v, mn_v, en_v, row_out, row_in, row_new = take(6)
    (in_sem, swap_s, rs_s, rs_r, ag_s, ag_r, agp_s, agp_r, mast_sem, half_s, half_r,
     sq_s, sq_r, pk_sem, pk_s, row_s, row_r, give_s, give_r) = take(19)

    r = lax.axis_index("replica")
    z, c = r // 2, r % 2
    peer = r + 1 - 2 * c
    x = lax.axis_index("model")
    chip = lambda off: lax.rem(z + off + 2 * Z, Z)
    beside = lambda d: {"replica": 2 * chip(STEP[d]) + c}
    across = lambda i: lax.rem(x + i, X)

    def remote(src, dst, s, rv, dev):
        return pltpu.make_async_remote_copy(src_ref=src, dst_ref=dst, send_sem=s, recv_sem=rv, device_id=dev, device_id_type=MESH)

    parts = (pg, pu, pd)

    def block(t, at, core):
        if t < 2:
            return parts[t].at[at, core]
        return pd.at[pl.ds(pl.multiple_of(HALF * core, HALF), HALF), pl.ds(pl.multiple_of(128 * at, 128), 128)]

    own_at = lambda t, at: own_gu.at[t, at] if t < 2 else own_d.at[at]
    peer_at = lambda t, at: peer_gu.at[t, at] if t < 2 else peer_d.at[at]
    ends = lambda lev: (lev,) if lev in (0, 4) else (lev, -lev)
    needed = []
    for code in ORDER:
        lev = int(code[3]) if code[0] == "r" else 0
        if code[0] in "rs" and (int(code[1]), lev) not in needed:
            needed.append((int(code[1]), lev))
    for t, lev in needed:
        for off in ends(lev):
            pltpu.make_async_copy(block(t, chip(off), c), own_at(t, chip(off)), in_sem.at[t, lev]).start()

    barrier = pltpu.get_barrier_semaphore()
    hello = [{"replica": peer}, beside(0), beside(1)]
    for i in range(1, X):
        hello.append({"model": across(i)})
        hello.append({"replica": peer, "model": across(i)})
    for dev in hello:
        pl.semaphore_signal(barrier, inc=1, device_id=dev, device_id_type=MESH)
    pl.semaphore_wait(barrier, len(hello))

    def await_in(ref, sem):
        remote(ref, ref, sem, sem, {"replica": peer}).wait_recv()

    def await_out(ref, sem):
        remote(ref, ref, sem, sem, {"replica": peer}).wait_send()

    swapped = []

    def swap(ahead):
        while len(swapped) < min(ahead, len(needed)):
            t, lev = needed[len(swapped)]
            for off in ends(lev):
                at = chip(off)
                remote(block(t, at, 1 - c), peer_at(t, at), swap_s.at[t // 2], in_sem.at[t, lev], {"replica": peer}).start()
            swapped.append((t, lev))

    have = []

    def need(t, lev):
        if (t, lev) not in have:
            have.append((t, lev))
            n = 2 * len(ends(lev))
            await_in(own_gu.at[0, pl.ds(0, n)] if t < 2 else own_d.at[pl.ds(0, n)], in_sem.at[t, lev])
            swap(len(have) + AHEAD)

    swap(AHEAD)

    half = lambda core: pl.ds(pl.multiple_of(HALF * core, HALF), HALF)
    mine, theirs = pl.ds(pl.multiple_of(64 * c, 64), 64), pl.ds(pl.multiple_of(64 * (1 - c), 64), 64)
    for t, pair in enumerate(((mg, eg), (mu, eu), (md, ed))):
        for i, ref in enumerate(pair):
            if t < 2:
                src, dst = ref, (mas_gu, mem_gu)[i].at[t]
            else:
                src, dst = ref.at[:, half(c)], (mas_d, mem_d)[i].at[mine]
                remote(ref.at[:, half(1 - c)], dst, half_s, half_r, {"replica": peer}).start()
            pltpu.make_async_copy(src, dst, mast_sem.at[t]).start()
    vectors = ((pn, pn_v), (mn, mn_v), (en, en_v))
    for j, (ref, buf) in enumerate(vectors):
        pltpu.make_async_copy(ref, buf.at[0], pk_sem.at[j]).start()
        remote(ref, buf.at[1], pk_s.at[j], pk_sem.at[j], {"replica": peer}).start()

    rs_out = lambda t, j: rs_out_gu.at[t, j] if t < 2 else rs_out_d.at[j]
    rs_in = lambda t, j: rs_in_gu.at[t, j] if t < 2 else rs_in_d.at[j]
    piece = lambda p, d: 1 - d if p == "L" else d

    size = lambda t: 16 if t < 2 else 96

    def rs_send(t, p, k):
        need(t, k)
        n, j = size(t), slot(p, k)
        chained = k < TOP[p]
        if chained:
            await_in(rs_in(t, j - 1), rs_r.at[t, j - 1])
        for d in range(2):
            at, h = chip(STEP[d] * k), piece(p, d)
            own, other, out = own_at(t, at), peer_at(t, at), rs_out(t, j).at[d]
            arrived = rs_in(t, j - 1).at[d] if chained else None

            def body(i, _):
                here = pl.ds(pl.multiple_of(i * n, n), n)
                there = pl.ds(pl.multiple_of(2 * n * h + i * n, n), n)
                v = own[there, :] + other[there, :]
                if chained:
                    v = v + decode(arrived[here, :])
                out[here, :] = encode(v)
                return 0

            lax.fori_loop(0, 2, body, 0)
            remote(out, rs_in(t, j).at[d], rs_s.at[t // 2], rs_r.at[t, j], beside(d)).start()

    def sq_slot(w, t):
        return sq_gu.at[w, t, x] if t < 2 else sq_d.at[w, 2 * x + c]

    def sq_copies(w, t):
        to = [{"model": across(i)} for i in range(1, X)]
        if t == 2:
            to += [{"replica": peer, "model": across(i)} for i in range(X)]
        return [remote(sq_slot(w, t), sq_slot(w, t), sq_s.at[t], sq_r.at[t], dev) for dev in to]

    def share(w, t):
        for copy in sq_copies(w, t):
            copy.start()

    sq_all = lambda t: sq_gu.at[:, t, pl.ds(0, X - 1)] if t < 2 else sq_d.at[:, pl.ds(0, 2 * X - 1)]

    def lanes(v):
        total = v[:, :128]
        for j in range(1, v.shape[1] // 128):
            total = total + v[:, 128 * j : 128 * (j + 1)]
        return total

    def eights(v):
        total = v[:8]
        for j in range(1, v.shape[0] // 8):
            total = total + v[8 * j : 8 * (j + 1)]
        return total

    def sum_up(t):
        need(t, 0)
        for p in "LS":
            await_in(rs_in(t, slot(p, 1)), rs_r.at[t, slot(p, 1)])
        n = size(t)
        own, other = own_at(t, z), peer_at(t, z)
        for h in range(2):
            ahead, back = (rs_in(t, slot("L" if piece("L", d) == h else "S", 1)).at[d] for d in range(2))

            def body(i, carry):
                here = pl.ds(pl.multiple_of(i * n, n), n)
                there = pl.ds(pl.multiple_of(2 * n * h + i * n, n), n)
                v = (own[there, :] + other[there, :]) + (decode(ahead[here, :]) + decode(back[here, :]))
                v = v * (2 * Z) ** -0.5
                if t < 2:
                    mean_gu[t, there, :] = v
                    sq_gu[0, t, x, there, :] = lanes(v * v)
                    return carry
                mean_d[there, :] = v
                return carry + eights(v * v)

            first = jnp.zeros((8, 128), F32) if h == 0 else total
            total = lax.fori_loop(0, 2, body, first)
        if t == 2:
            sq_d[0, 2 * x + c] = total
        share(0, t)

    def master(t):
        await_in(mean_gu if t < 2 else mas_d, mast_sem.at[t])
        if t < 2:

            def body(i, _):
                here = pl.ds(pl.multiple_of(16 * i, 16), 16)
                v = mas_gu[t, here, :]
                sq_gu[1, t, x, here, :] = lanes(v * v)
                return 0

            lax.fori_loop(0, 4, body, 0)
        else:
            await_in(mas_d, half_r)

            def body(i, carry):
                v = mas_d[:, pl.ds(pl.multiple_of(128 * i, 128), 128)]
                return carry + v * v

            total = lax.fori_loop(0, HALF // 128, body, jnp.zeros((128, 128), F32))
            sq_d[1, 2 * x + c] = eights(total.T)
        share(1, t)

    def update(t):
        await_in(sq_all(t), sq_r.at[t])
        if t < 2:

            def body(i, _):
                here = pl.ds(pl.multiple_of(16 * i, 16), 16)

                def whole(w):
                    total = sq_gu[w, t, 0, here, :]
                    for j in range(1, X):
                        total = total + sq_gu[w, t, j, here, :]
                    return jnp.sum(total, axis=1, keepdims=True)

                ratio = jnp.sqrt(whole(1)) * lax.rsqrt(whole(0) + 1e-6)
                state = hold_rate * mem_gu[t, here, :] + mean_gu[t, here, :] * ratio
                stepped = mas_gu[t, here, :] - learn_rate * state
                (sg, su)[t][here, :] = stepped
                (tg, tu)[t][here, :] = state
                (cg, cu)[t][z, c, here, :] = stepped.astype(BF16)
                return 0

            lax.fori_loop(0, 4, body, 0)
        else:

            def whole(w):
                total = sq_d[w, 0]
                for j in range(1, 2 * X):
                    total = total + sq_d[w, j]
                return jnp.sum(total, axis=0, keepdims=True)

            ratio = jnp.sqrt(whole(1)) * lax.rsqrt(whole(0) + 1e-6)

            def body(i, _):
                here = pl.ds(pl.multiple_of(128 * i, 128), 128)
                state = hold_rate * mem_d[:, here] + (mean_d[here, :] * ratio).T
                stepped = mas_d[:, here] - learn_rate * state
                cd[z, c, here, :] = stepped.T.astype(BF16)
                there = pl.ds(pl.multiple_of(HALF * c + 128 * i, 128), 128)
                for j, v in enumerate((stepped, state)):
                    (sd, td)[j][:, there] = jnp.where(low_core, v[:64], v[64:])
                    give_d[j, :, here] = jnp.where(low_core, v[64:], v[:64])
                return 0

            low_core = lax.broadcast_in_dim(c, (64, 128), ()) == 0
            lax.fori_loop(0, HALF // 128, body, 0)
        for p in "LS":
            ag_send(t, p, 1)
        for h in range(2):
            deliver(t, 0, h)
        if t == 2:
            for j, ref in enumerate((sd, td)):
                remote(give_d.at[j], ref.at[:, half(c)], give_s, give_r, {"replica": peer}).start()


    def ag_at(t, at, h):
        return (cg, cu, cd)[t].at[at, c, pl.ds((32, 32, 192)[t] * h, (32, 32, 192)[t])]

    def deliver(t, off, h):
        at = ag_at(t, chip(off), h)
        remote(at, at, agp_s.at[t], agp_r.at[t], {"replica": peer}).start()

    def ag_send(t, p, k):
        for d in range(2):
            at = ag_at(t, chip(-STEP[d] * (k - 1)), piece(p, d))
            remote(at, at, ag_s.at[t], ag_r.at[t, slot(p, k)], beside(d)).start()

    def ag_step(t, p, k):
        await_in((cg, cu, cd)[t].at[0, 0], ag_r.at[t, slot(p, k - 1)])
        if k <= TOP[p]:
            ag_send(t, p, k)
        for d in range(2):
            deliver(t, -STEP[d] * (k - 1), piece(p, d))

    turn = lambda v: jnp.concatenate([v[:, 64:], v[:, :64]], axis=1)
    core0 = lambda n: lax.broadcast_in_dim(c, (1, n), ()) == 0

    def rows_to(src, dst, j):
        for off in range(1, Z):
            remote(src(off), dst.at[z], row_s.at[j], row_r.at[j], {"replica": 2 * chip(off) + c}).start()

    def norm_parts():
        for j, (_, buf) in enumerate(vectors):
            await_in(buf, pk_sem.at[j])
        for j in range(Z):
            row_out[j] = pn_v[0, j : j + 1, :] + pn_v[1, j : j + 1, :]
        row_in[z] = row_out[z]
        rows_to(lambda off: row_out.at[chip(off)], row_in, 0)

    def norm_step():
        await_in(row_out.at[pl.ds(0, Z - 1)], row_r.at[0])
        total = row_in[0]
        for j in range(1, Z):
            total = total + row_in[j]

        def both(ref):
            a, b = jnp.concatenate([ref[0], ref[1]], axis=1), jnp.concatenate([ref[1], ref[0]], axis=1)
            return jnp.where(core0(128), a, b)

        state = hold_rate * both(en_v) + total * (2 * Z) ** -0.5
        stepped = both(mn_v) - learn_rate * state
        row_new[z] = stepped
        rows_to(lambda off: row_new.at[z], row_new, 1)
        sn[...] = jnp.where(core0(64), stepped[:, :64], turn(stepped)[:, :64])
        tn[...] = jnp.where(core0(64), state[:, :64], turn(state)[:, :64])

    def norm_all():
        await_in(row_out.at[pl.ds(0, Z - 1)], row_r.at[1])
        cn[...] = jnp.concatenate([row_new[j] for j in range(Z)], axis=0).astype(BF16)

    for code in ORDER:
        kind, t = code[0], int(code[1])
        with jax.named_scope(code):
            if kind == "r":
                rs_send(t, code[2], int(code[3]))
            elif kind == "a":
                ag_step(t, code[2], int(code[3]))
            elif kind == "n":
                (norm_parts, norm_step, norm_all)[t]()
            else:
                {"s": sum_up, "m": master, "u": update}[kind](t)

    for t in range(3):
        await_in((cg, cu, cd)[t].at[:, 0], agp_r.at[t])
    await_in(give_d, give_r)
    for j in range(2):
        await_out((peer_gu, peer_d)[j], swap_s.at[j])
        await_out((rs_out_gu, rs_out_d)[j], rs_s.at[j])
    for t in range(3):
        await_out((cg, cu, cd)[t].at[pl.ds(0, 7), 0], ag_s.at[t])
        await_out((cg, cu, cd)[t].at[:, 0], agp_s.at[t])
        await_out(sq_all(t), sq_s.at[t])
    await_out(mas_d, half_s)
    for j, (ref, buf) in enumerate(vectors):
        await_out(buf.at[1], pk_s.at[j])
    for j in range(2):
        await_out(row_out.at[pl.ds(0, Z - 1)], row_s.at[j])
    await_out(give_d, give_s)


def write(*refs):
    src, dst, sem = refs[:12], refs[12:24], refs[24]
    copies = []

    for at in range(Z):
        for core in range(2):
            there = dst[2].at[pl.ds(HALF * core, HALF), pl.ds(128 * at, 128)]
            pltpu.make_async_copy(src[2].at[at, core], there, sem.at[2]).start()
    for i in range(12):
        if i != 2:
            copies.append(pltpu.make_async_copy(src[i], dst[i], sem.at[i]))
            copies[-1].start()
    for copy in copies:
        copy.wait()
    pltpu.make_async_copy(dst[2], dst[2], sem.at[2]).wait()


def call(*args):
    S = jax.ShapeDtypeStruct
    dma = pltpu.SemaphoreType.DMA
    outs = (
        S((Z, 2, ROWS, COLS), BF16), S((Z, 2, ROWS, COLS), BF16), S((Z, 2, HALF, 128), BF16), S((8, 128), BF16),
        S((ROWS, COLS), F32), S((ROWS, COLS), F32), S((64, 2 * HALF), F32), S((1, 64), F32),
        S((ROWS, COLS), F32), S((ROWS, COLS), F32), S((64, 2 * HALF), F32), S((1, 64), F32),
    )
    v = pltpu.VMEM
    scratch = [
        v((2, Z, ROWS, COLS), F32), v((2, Z, ROWS, COLS), F32), v((Z, HALF, 128), F32), v((Z, HALF, 128), F32),
        v((2, 7, 2, 32, COLS), BF16), v((2, 7, 2, 32, COLS), BF16), v((7, 2, 192, 128), BF16), v((7, 2, 192, 128), BF16),
        v((2, ROWS, COLS), F32), v((HALF, 128), F32),
        v((2, ROWS, COLS), F32), v((2, ROWS, COLS), F32), v((128, HALF), F32), v((128, HALF), F32),
        v((2, 64, HALF), F32),
        v((2, 2, X, ROWS, 128), F32), v((2, 2 * X, 8, 128), F32),
        v((2, 8, 128), F32), v((2, 1, 64), F32), v((2, 1, 64), F32), v((Z, 1, 128), F32), v((Z, 1, 128), F32), v((Z, 1, 128), F32),
        dma((3, 5)), dma((2,)), dma((2,)), dma((3, 7)), dma((3,)), dma((3, 7)), dma((3,)), dma((3,)), dma((3,)), dma(()), dma(()),
        dma((3,)), dma((3,)), dma((3,)), dma((3,)), dma((2,)), dma((2,)), dma(()), dma(()),
    ]
    any_, hbm = pl.BlockSpec(memory_space=pl.ANY), pl.BlockSpec(memory_space=pltpu.HBM)
    args = [pltpu.with_memory_space_constraint(a, pltpu.HBM) for a in args]
    results = pl.pallas_call(
        kernel,
        out_shape=outs,
        in_specs=[hbm] * len(args),
        out_specs=[pl.BlockSpec(memory_space=pltpu.VMEM)] * len(outs),
        scratch_shapes=scratch,
        compiler_params=pltpu.CompilerParams(collective_id=0, has_side_effects=True, vmem_limit_bytes=28 * 2**20),
    )(*args)
    return pl.pallas_call(
        write,
        out_shape=outs[:2] + (S((2 * HALF, 128 * Z), BF16),) + outs[3:],
        in_specs=[any_] * len(outs),
        out_specs=[hbm] * len(outs),
        scratch_shapes=[dma((12,))],
        compiler_params=pltpu.CompilerParams(vmem_limit_bytes=2**20),
    )(*results)


def on_device(pg, pu, pd, pn, mg, mu, md, mn, eg, eu, ed, en):
    wide = lambda p: p.reshape(Z, 2, ROWS, COLS)
    cg, cu, cd, cn, sg, su, sd, sn, tg, tu, td, tn = call(
        wide(pg), wide(pu), pd[0], pn.reshape(8, 128), mg, mu, md.T, mn.reshape(1, -1), eg, eu, ed.T, en.reshape(1, -1)
    )
    flat = (2 * Z * ROWS, COLS)
    return (cg.reshape(flat), cu.reshape(flat), cd, cn.reshape(-1), sg, su, sd.T, sn[0], tg, tu, td.T, tn[0])


def solution(mesh):
    rows, cols = P(("shift", "replica"), "model"), P(("shift", "model"), "replica")
    vec = P(("shift", "replica"))
    return jax.shard_map(
        on_device,
        mesh=mesh,
        in_specs=(
            P(("shift", "replica"), None, "model"), P(("shift", "replica"), None, "model"), P(("shift", "replica"), "model", None),
            P(("shift", "replica"), None), rows, rows, cols, vec, rows, rows, cols, vec,
        ),
        out_specs=(
            P("shift", "model"), P("shift", "model"), P(("shift", "model"), None), P("shift"),
            rows, rows, cols, vec, rows, rows, cols, vec,
        ),
        check_vma=False,
    )
```
